32 devices in a mesh: seq: 4 (over z), grp: 8 (over y, x, core).
Axes of the slice: x: 2, y: 2, z: 4, core: 2. Of those that a mesh axis runs over, the one named last changes fastest.
Arguments:
- hidden_in: bfloat16 [8, 2048, 1024], P('grp', 'seq'), may hold values from -64 to 64, as said below
- lengths: int32 [8], P('grp'), may hold values from 256 to 2048
- project_weight: bfloat16 [1024, 3072], replicated, may hold values from -0.1875 to 0.1875
- output_weight: bfloat16 [1024, 1024], replicated, may hold values from -0.1875 to 0.1875
- first_gain: float32 [1024], replicated, may hold values from 0.5 to 1.5
- first_shift: float32 [1024], replicated, may hold values from -3 to 3
- up_weight: bfloat16 [1024, 4096], P('grp'), may hold values from -0.1875 to 0.1875
- down_weight: bfloat16 [1024, 4096], P('grp'), may hold values from -0.09375 to 0.09375
- second_gain: float32 [1024], replicated, may hold values from 0.5 to 1.5
- second_shift: float32 [1024], replicated, may hold values from -3 to 3
- queries: float32 [64, 1024], P('grp'), may hold values from -6 to 6
- positive: int32 [64], P('grp'), may hold values from 0 to 7
Outputs:
- hidden_out: bfloat16 [8, 2048, 1024], P('grp', 'seq')
- embeddings: float32 [8, 1024], P('grp')
- query_loss: float32 [64], P('grp')
The draws below stay inside these ranges and needn't reach their ends.
Inputs may be any that keep to these rules, and one draw needn't show every extreme that they name: `hidden_in`: activations.
All inputs are finite; a program needn't handle non-finite values.
Results may differ from the reference program's by a relative error of at most 0.0076.
Values may be sent and summed in bfloat16 or wider, within the bound.
No kernel may reach another device: no remote copies, remote signals or barrier semaphores. Data moves between devices by JAX's collectives and lax.ppermute only.
A program may use at most 192 MiB of HBM per device.

```python
import math
import jax
import jax.numpy as jnp
from jax import lax

D = 1024
HEADS = 16
HEAD_DIM = 64
FF = 4096
LEN = 2048
PASSAGES = 8
QUERIES = 64


def draw_hidden_in(key, part):
    base = jnp.clip(jax.random.normal(key, (PASSAGES, LEN, D), jnp.float32), -6.0, 6.0)
    return base.astype(jnp.bfloat16)


def plant(drawn, own_key, least, high):
    spot = [jax.random.randint(jax.random.fold_in(own_key, axis), (), 0, length) for axis, length in enumerate(drawn.shape)]
    main_axis = drawn.shape.index(max(drawn.shape))
    neighbour = spot[:main_axis] + [(spot[main_axis] + 1) % drawn.shape[main_axis]] + spot[main_axis + 1:]
    return drawn.at[tuple(spot)].set(least).at[tuple(neighbour)].set(high)


def shard_levels(stream_key, dims, shards, low, top_value):
    def one(position, parts):
        draws = jax.random.uniform(jax.random.fold_in(jax.random.fold_in(stream_key, 6), position), (parts,), jnp.float32, low / len(shards), top_value / len(shards))
        return jnp.repeat(jnp.exp(draws), dims[position] // parts).reshape((-1,) + (1,) * (len(dims) - position - 1))

    factor_of = one(*shards[0])
    for cut in shards[1:]:
        factor_of = factor_of * one(*cut)
    return factor_of


def bell_draw(stream_key, dims, width, most, shards=(), kind=jnp.bfloat16):
    level = shard_levels(stream_key, dims, shards, -0.22, 0.18) if shards else 1.0
    values = jax.random.normal(stream_key, dims, jnp.float32) * width * level
    return jnp.minimum(jnp.maximum(values, -most), most).astype(kind)


def setup_inputs(seed: int = 0) -> dict:
    arg_keys = jax.random.split(jax.random.key(seed), 13)
    hidden_in = draw_hidden_in(jax.random.fold_in(arg_keys[12], 71), 0)
    lengths = plant(jax.random.randint(arg_keys[1], (PASSAGES,), LEN // 8, LEN + 1), jax.random.fold_in(arg_keys[1], 1), LEN // 8, LEN).astype(jnp.int32)
    project_weight = bell_draw(arg_keys[2], (D, 3 * D), D ** -0.5, 0.1875)
    output_weight = bell_draw(arg_keys[3], (D, D), D ** -0.5, 0.1875)
    first_gain = jnp.clip(1.0 + 0.1 * jax.random.normal(arg_keys[4], (D,), jnp.float32), 0.5, 1.5)
    first_shift = bell_draw(arg_keys[5], (D,), 0.5, 3.0, (), jnp.float32)
    up_weight = bell_draw(arg_keys[6], (D, FF), D ** -0.5, 0.1875, ((0, 8),))
    down_weight = bell_draw(arg_keys[7], (D, FF), FF ** -0.5, 0.09375, ((0, 8),))
    second_gain = jnp.clip(1.0 + 0.1 * jax.random.normal(arg_keys[8], (D,), jnp.float32), 0.5, 1.5)
    second_shift = bell_draw(arg_keys[9], (D,), 0.5, 3.0, (), jnp.float32)
    queries = bell_draw(arg_keys[10], (QUERIES, D), 1.0, 6.0, ((0, 8),), jnp.float32)
    positive = plant(jax.random.randint(arg_keys[11], (QUERIES,), 0, PASSAGES), jax.random.fold_in(arg_keys[11], 1), 0, PASSAGES - 1).astype(jnp.int32)
    return {"hidden_in": hidden_in, "lengths": lengths, "project_weight": project_weight, "output_weight": output_weight, "first_gain": first_gain, "first_shift": first_shift, "up_weight": up_weight, "down_weight": down_weight, "second_gain": second_gain, "second_shift": second_shift, "queries": queries, "positive": positive}


def layer_norm(values, gain, shift):
    average = lax.optimization_barrier(jnp.mean(values, axis=-1, keepdims=True))
    centred = values - average
    variance = lax.optimization_barrier(jnp.mean(centred * centred, axis=-1, keepdims=True))
    return centred * lax.rsqrt(variance + 1e-05) * gain + shift

def attend(projected, length):
    block = min(1024, LEN)
    query_all = projected[:, :D].reshape(LEN, HEADS, HEAD_DIM).astype(jnp.float32)
    key_all = projected[:, D:2 * D].reshape(LEN, HEADS, HEAD_DIM).astype(jnp.float32)
    value_all = projected[:, 2 * D:].reshape(LEN, HEADS, HEAD_DIM).astype(jnp.float32)
    key_valid = jnp.arange(LEN, dtype=jnp.int32) < length
    scale = 1.0 / math.sqrt(HEAD_DIM)

    def one_block(index):
        query_rows = lax.dynamic_slice_in_dim(query_all, (index * block).astype(jnp.int32), block, 0)
        scores = jnp.einsum('qhd,khd->hqk', query_rows, key_all) * scale
        scores = jnp.where(key_valid[None, None, :], scores, -jnp.inf)
        highest = lax.optimization_barrier(jnp.max(scores, axis=-1, keepdims=True))
        expo = jnp.exp(scores - highest)
        probs = (expo / lax.optimization_barrier(jnp.sum(expo, axis=-1, keepdims=True))).astype(jnp.bfloat16)
        result = jnp.einsum('hqk,khd->qhd', probs.astype(jnp.float32), value_all)
        return result.astype(jnp.bfloat16).reshape(block, D)
    blocks = lax.map(one_block, jnp.arange(LEN // block, dtype=jnp.int32))
    return blocks.reshape(LEN, D)

def reference(hidden_in, lengths, project_weight, output_weight, first_gain, first_shift, up_weight, down_weight, second_gain, second_shift, queries, positive):

    def encode(item):
        tokens, length = item
        projected = jnp.dot(tokens, project_weight, preferred_element_type=jnp.float32).astype(jnp.bfloat16)
        attended = attend(projected, length)
        mixed = jnp.dot(attended, output_weight, preferred_element_type=jnp.float32) + tokens.astype(jnp.float32)
        normed = layer_norm(mixed, first_gain, first_shift).astype(jnp.bfloat16)
        inner = jax.nn.gelu(jnp.dot(normed, up_weight, preferred_element_type=jnp.float32), approximate=False).astype(jnp.bfloat16)
        outer = lax.dot_general(inner, down_weight, (((1,), (1,)), ((), ())), preferred_element_type=jnp.float32)
        final = layer_norm(outer + normed.astype(jnp.float32), second_gain, second_shift)
        valid = (jnp.arange(LEN, dtype=jnp.int32) < length).astype(jnp.float32)
        pooled = lax.optimization_barrier(jnp.sum(final * valid[:, None], axis=0)) / length.astype(jnp.float32)
        return (final.astype(jnp.bfloat16), pooled)
    hidden_out, pooled = lax.map(encode, (hidden_in, lengths))
    embeddings = pooled / jnp.sqrt(lax.optimization_barrier(jnp.sum(pooled * pooled, axis=-1, keepdims=True)) + 1e-06)
    short_queries = (queries / jnp.sqrt(lax.optimization_barrier(jnp.sum(queries * queries, axis=-1, keepdims=True)) + 1e-06)).astype(jnp.bfloat16)
    short_passages = embeddings.astype(jnp.bfloat16)
    logits = 20.0 * jnp.dot(short_queries, short_passages.T, preferred_element_type=jnp.float32)
    chosen = positive[:, None] == jnp.arange(PASSAGES, dtype=jnp.int32)[None, :]
    picked = lax.optimization_barrier(jnp.sum(jnp.where(chosen, logits, 0.0), axis=1))
    query_loss = jnp.log(lax.optimization_barrier(jnp.sum(jnp.exp(logits), axis=1))) - picked
    return (hidden_out, embeddings, query_loss)
```

```python
import functools
import math

import jax
import jax.numpy as jnp
from jax import lax
from jax.experimental import pallas as pl
from jax.experimental.pallas import tpu as pltpu
from jax.sharding import PartitionSpec as P

HEAD_DIM = 64
QUAD = 4
ROWS = HEAD_DIM + 16
LOW = -1e30
EPS = 1e-05
F32 = jnp.float32
BF16 = jnp.bfloat16


def dot(a, b):
    return jnp.dot(a, b, preferred_element_type=F32)


def key_bias(first, length, count):
    place = first + lax.broadcasted_iota(jnp.int32, (count, 128), 0)
    lane = lax.broadcasted_iota(jnp.int32, (count, 128), 1)
    return jnp.where((lane == 0) & (place >= length), LOW, 0.0).astype(BF16)


def attend_chunk(x, wk, wv, qt_ref, bias, state_in, state_out):
    count = x.shape[0]
    tok = qt_ref.shape[1]
    k = dot(x, wk).astype(BF16)
    vt = dot(x, wv).T.astype(BF16)
    ones = jnp.ones((16, count), BF16)
    zeros = jnp.zeros((HEAD_DIM, tok), BF16)
    pick = (lax.broadcasted_iota(jnp.int32, (128, tok), 0) == 0).astype(F32).astype(BF16)
    for h in range(QUAD):
        pair = h // 2
        keys = jnp.concatenate([k[:, pair * 128 : (pair + 1) * 128], bias], axis=1)
        q = qt_ref[h * HEAD_DIM : (h + 1) * HEAD_DIM, :]
        halves = [q, zeros] if h % 2 == 0 else [zeros, q]
        scores = dot(keys, jnp.concatenate(halves + [pick], axis=0))
        top = jnp.max(scores, axis=0, keepdims=True)
        if state_in is not None:
            old = state_in[h, HEAD_DIM + 8 : HEAD_DIM + 9, :]
            top = jnp.maximum(top, old)
        expo = jnp.exp2(scores - top).astype(BF16)
        values = jnp.concatenate([vt[h * HEAD_DIM : (h + 1) * HEAD_DIM, :], ones], axis=0)
        part = dot(values, expo)[: HEAD_DIM + 8]
        if state_in is not None:
            part = part + state_in[h, : HEAD_DIM + 8, :] * jnp.exp2(old - top)
        state_out[h, : HEAD_DIM + 8, :] = part
        state_out[h, HEAD_DIM + 8 :, :] = jnp.broadcast_to(top, (8, tok))


def first_kernel(info, x_ref, wq, wk, wv, qt_ref, state_ref):
    x = x_ref[...]
    scale = math.log2(math.e) / math.sqrt(HEAD_DIM)
    qt_ref[...] = (dot(x, wq[...]) * scale).T.astype(BF16)
    bias = key_bias(info[0], info[1], x.shape[0])
    attend_chunk(x, wk[...], wv[...], qt_ref, bias, None, state_ref)


def next_kernel(info, xr_ref, xl_ref, wk, wv, qt_ref, state_in, state_ref):
    count = xr_ref.shape[0]
    length = info[4]
    state_ref[...] = state_in[...]
    for side, x_ref in ((0, xr_ref), (1, xl_ref)):

        @pl.when(info[2 * side] > 0)
        def _():
            bias = key_bias(info[2 * side + 1], length, count)
            attend_chunk(x_ref[...], wk[...], wv[...], qt_ref, bias, state_ref, state_ref)


def grid_params(mib):
    return pltpu.CompilerParams(
        dimension_semantics=("arbitrary",), vmem_limit_bytes=mib * 1024 * 1024
    )


def attend_specs(tok, width):
    groups = width // (QUAD * HEAD_DIM)
    cols = QUAD * HEAD_DIM
    info = pl.BlockSpec(memory_space=pltpu.SMEM)
    full = pl.BlockSpec((tok, width), lambda j: (0, 0))
    weight = [
        pl.BlockSpec((width, cols), functools.partial(lambda s, j: (0, s * groups + j), s))
        for s in range(3)
    ]
    qt = pl.BlockSpec((cols, tok), lambda j: (j, 0))
    state = pl.BlockSpec((QUAD, ROWS, tok), lambda j: (j, 0, 0))
    return groups, info, full, weight, qt, state


def attend_cost(tok, width, chunks):
    return pl.CostEstimate(
        flops=chunks * (2 * tok * width * width * 3 + 16 * tok * tok * width),
        bytes_accessed=8 * tok * width,
        transcendentals=chunks * tok * tok * width // HEAD_DIM,
    )


def attend_first(x, weight, info):
    tok, width = x.shape
    groups, s_info, s_x, s_w, s_q, s_state = attend_specs(tok, width)
    return pl.pallas_call(
        first_kernel,
        grid=(groups,),
        in_specs=[s_info, s_x] + s_w,
        out_specs=[s_q, s_state],
        out_shape=[
            jax.ShapeDtypeStruct((width, tok), BF16),
            jax.ShapeDtypeStruct((width // HEAD_DIM, ROWS, tok), F32),
        ],
        compiler_params=grid_params(40),
        cost_estimate=attend_cost(tok, width, 1),
        name="attend_first",
    )(info, x, weight, weight, weight)


def attend_next(xr, xl, weight, qt, state, info, index):
    tok, width = xr.shape
    groups, s_info, s_x, s_w, s_q, s_state = attend_specs(tok, width)
    return pl.pallas_call(
        next_kernel,
        grid=(groups,),
        in_specs=[s_info, s_x, s_x, s_w[1], s_w[2], s_q, s_state],
        out_specs=s_state,
        out_shape=jax.ShapeDtypeStruct(state.shape, F32),
        compiler_params=grid_params(40),
        cost_estimate=attend_cost(tok, width, 1),
        name=f"attend_next_{index}",
    )(info, xr, xl, weight, weight, qt, state)


def layer_norm(values, gain, shift):
    average = jnp.mean(values, axis=-1, keepdims=True)
    centred = values - average
    variance = jnp.mean(centred * centred, axis=-1, keepdims=True)
    return centred * lax.rsqrt(variance + EPS) * gain + shift


def mix_kernel(state_ref, wo, x_ref, gain, shift, out_ref):
    heads = state_ref.shape[0]
    columns = []
    for h in range(heads):
        block = state_ref[h]
        columns.append(block[:HEAD_DIM] / block[HEAD_DIM : HEAD_DIM + 1])
    attended = jnp.concatenate(columns, axis=0).T.astype(BF16)
    mixed = dot(attended, wo[...]) + x_ref[...].astype(F32)
    out_ref[...] = layer_norm(mixed, gain[...], shift[...]).astype(BF16)


def mix(state, wo, x, gain, shift):
    return pl.pallas_call(
        mix_kernel,
        out_shape=jax.ShapeDtypeStruct(x.shape, BF16),
        compiler_params=pltpu.CompilerParams(vmem_limit_bytes=40 * 1024 * 1024),
        cost_estimate=pl.CostEstimate(
            flops=2 * x.shape[0] * x.shape[1] ** 2, bytes_accessed=2**23, transcendentals=0
        ),
        name="mix",
    )(state, wo, x, gain, shift)


def feed_kernel(plan, width_cols, info, normed_ref, gain, shift, *refs):
    count = len(plan)
    ups, downs = refs[:count], refs[count : 2 * count]
    out_ref, pooled_ref, up_v, down_v, inner, up_sem, down_sem = refs[2 * count :]
    tok, width = normed_ref.shape
    ff = up_v.shape[1]
    shard = info[0]
    rows_each = plan[0][1] if plan[0][0] == 0 else None
    chunks = ff // width_cols

    def up_copy(c, i):
        mask, rows, offset = plan[i]
        start = pl.multiple_of(jnp.bitwise_xor(shard, mask) * rows_each + offset, 64)
        return pltpu.make_async_copy(
            ups[i].at[:, pl.ds(c * width_cols, width_cols)],
            up_v.at[pl.ds(start, rows), pl.ds(c * width_cols, width_cols)],
            up_sem.at[c, i],
        )

    def down_copy(i):
        mask, rows, offset = plan[i]
        start = pl.multiple_of(jnp.bitwise_xor(shard, mask) * rows_each + offset, 64)
        return pltpu.make_async_copy(
            downs[i], down_v.at[pl.ds(start, rows), :], down_sem.at[i]
        )

    for c in range(chunks):
        for i in range(count):
            up_copy(c, i).start()
    for i in range(count):
        down_copy(i).start()
    for c in range(chunks):
        for i in range(count):
            up_copy(c, i).wait()
        cols = slice(c * width_cols, (c + 1) * width_cols)
        pre = dot(normed_ref[...], up_v[:, cols])
        inner[:, cols] = (0.5 * pre * (1.0 + lax.erf(pre * math.sqrt(0.5)))).astype(BF16)
    for i in range(count):
        down_copy(i).wait()
    outer = lax.dot_general(
        inner[...], down_v[...], (((1,), (1,)), ((), ())), preferred_element_type=F32
    )
    final = layer_norm(outer + normed_ref[...].astype(F32), gain[...], shift[...])
    out_ref[...] = final.astype(BF16)
    place = info[1] + lax.broadcasted_iota(jnp.int32, (tok, 1), 0)
    total = jnp.sum(jnp.where(place < info[2], final, 0.0), axis=0, keepdims=True)
    pooled_ref[...] = total / info[2].astype(F32)


def feed(normed, gain, shift, ups, downs, plan, info):
    tok, width = normed.shape
    ff = ups[0].shape[1]
    cols = min(1024, ff)
    vmem = pl.BlockSpec(memory_space=pltpu.VMEM)
    anyspace = pl.BlockSpec(memory_space=pl.ANY)
    return pl.pallas_call(
        functools.partial(feed_kernel, plan, cols),
        in_specs=[pl.BlockSpec(memory_space=pltpu.SMEM), vmem, vmem, vmem]
        + [anyspace] * (2 * len(plan)),
        out_specs=[vmem, vmem],
        out_shape=[
            jax.ShapeDtypeStruct((tok, width), BF16),
            jax.ShapeDtypeStruct((1, width), F32),
        ],
        scratch_shapes=[
            pltpu.VMEM((width, ff), BF16),
            pltpu.VMEM((width, ff), BF16),
            pltpu.VMEM((tok, ff), BF16),
            pltpu.SemaphoreType.DMA((ff // cols, len(plan))),
            pltpu.SemaphoreType.DMA((len(plan),)),
        ],
        compiler_params=pltpu.CompilerParams(vmem_limit_bytes=52 * 1024 * 1024),
        cost_estimate=pl.CostEstimate(
            flops=4 * tok * width * ff, bytes_accessed=4 * width * ff, transcendentals=tok * ff
        ),
        name="feed",
    )(info, normed, gain, shift, *ups, *downs)


def gather_rows(part, axis, size):
    rows = part.shape[0]
    half = rows // 2
    bits = [1 << b for b in range(size.bit_length() - 1)]

    def swap(values, mask):
        return lax.ppermute(values, axis, [(i, i ^ mask) for i in range(size)])

    found = [(0, rows, 0, part)]
    if len(bits) >= 3:
        one, two = bits[1], bits[2]
        rest = [b for b in bits if b not in (one, two)]
        a = swap(part, one)
        b = swap(part, two)
        c = swap(b[:half], one)
        d = swap(a[half:], two)
        found += [(one, rows, 0, a), (two, rows, 0, b)]
        found += [(one | two, half, 0, c), (one | two, rows - half, half, d)]
    else:
        rest = bits
    for bit in rest:
        found += [(m | bit, r, o, swap(v, bit)) for m, r, o, v in found]
    return tuple(f[:3] for f in found), [f[3] for f in found]


def line_shift(values, axis, size, step):
    pairs = [(i, i + step) for i in range(size) if 0 <= i + step < size]
    return lax.ppermute(values, axis, pairs)


def body(
    n_seq,
    n_grp,
    hidden_in,
    lengths,
    project_weight,
    output_weight,
    first_gain,
    first_shift,
    up_weight,
    down_weight,
    second_gain,
    second_shift,
    queries,
    positive,
):
    tokens = hidden_in[0]
    tok_rows, width = tokens.shape
    rank = lax.axis_index("seq")
    shard = lax.axis_index("grp")
    length = lengths[0]

    right = left = tokens
    arrived = []
    for step in range(1, n_seq):
        with jax.named_scope(f"right_{step}"):
            right = line_shift(right, "seq", n_seq, 1)
        with jax.named_scope(f"left_{step}"):
            left = line_shift(left, "seq", n_seq, -1)
        arrived.append((right, left))
    plan, ups = gather_rows(up_weight, "grp", n_grp)
    _, downs = gather_rows(down_weight, "grp", n_grp)

    info = jnp.stack([rank * tok_rows, length]).astype(jnp.int32)
    qt, state = attend_first(tokens, project_weight, info)
    for step, (right, left) in enumerate(arrived, 1):
        info = jnp.stack(
            [
                (rank >= step).astype(jnp.int32),
                (rank - step) * tok_rows,
                (rank + step < n_seq).astype(jnp.int32),
                (rank + step) * tok_rows,
                length,
            ]
        ).astype(jnp.int32)
        state = attend_next(right, left, project_weight, qt, state, info, step)
    normed = mix(state, output_weight, tokens, first_gain[None], first_shift[None])
    info = jnp.stack([shard, rank * tok_rows, length]).astype(jnp.int32)
    final, part = feed(
        normed, second_gain[None], second_shift[None], ups, downs, plan, info
    )
    pooled = lax.psum(part, "seq")
    embedding = pooled / jnp.sqrt(jnp.sum(pooled * pooled) + 1e-06)
    short_passages = lax.all_gather(embedding.astype(BF16), "grp", axis=0, tiled=True)
    short_queries = (
        queries / jnp.sqrt(jnp.sum(queries * queries, axis=-1, keepdims=True) + 1e-06)
    ).astype(BF16)
    logits = 20.0 * jnp.dot(short_queries, short_passages.T, preferred_element_type=F32)
    passage_ids = jnp.arange(short_passages.shape[0], dtype=jnp.int32)
    chosen = positive[:, None] == passage_ids[None, :]
    picked = jnp.sum(jnp.where(chosen, logits, 0.0), axis=1)
    query_loss = jnp.log(jnp.sum(jnp.exp(logits), axis=1)) - picked
    return (final[None], embedding, query_loss)


def solution(mesh):
    in_specs = (
        P("grp", "seq", None),
        P("grp"),
        P(),
        P(),
        P(),
        P(),
        P("grp", None),
        P("grp", None),
        P(),
        P(),
        P("grp", None),
        P("grp"),
    )
    out_specs = (P("grp", "seq", None), P("grp", None), P("grp"))
    run = functools.partial(body, mesh.shape["seq"], mesh.shape["grp"])
    return jax.shard_map(run, mesh=mesh, in_specs=in_specs, out_specs=out_specs, check_vma=False)
```

```python
import functools
import math

import jax
import jax.numpy as jnp
from jax import lax
from jax.experimental import pallas as pl
from jax.experimental.pallas import tpu as pltpu
from jax.sharding import PartitionSpec as P


HEAD_DIM = 64
HEADS_STEP = 8
ROWS = HEAD_DIM + 16
LOW = -1e30
EPS = 1e-05
F32 = jnp.float32
BF16 = jnp.bfloat16


def dot(a, b):
    return jnp.dot(a, b, preferred_element_type=F32)


def key_bias(first, length, count):
    place = first + lax.broadcasted_iota(jnp.int32, (count, 128), 0)
    lane = lax.broadcasted_iota(jnp.int32, (count, 128), 1)
    return jnp.where((lane == 0) & (place >= length), LOW, 0.0).astype(BF16)


def attend_chunk(x, wk, wv, qt_ref, bias, state_in, state_out):
    count = x.shape[0]
    tok = qt_ref.shape[1]
    heads = qt_ref.shape[0] // HEAD_DIM
    k = dot(x, wk).astype(BF16)
    vt = dot(x, wv).T.astype(BF16)
    ones = jnp.ones((16, count), BF16)
    zeros = jnp.zeros((HEAD_DIM, tok), BF16)
    pick = (lax.broadcasted_iota(jnp.int32, (128, tok), 0) == 0).astype(F32).astype(BF16)

    def score(h):
        pair = h // 2
        keys = jnp.concatenate([k[:, pair * 128 : (pair + 1) * 128], bias], axis=1)
        q = qt_ref[h * HEAD_DIM : (h + 1) * HEAD_DIM, :]
        halves = [q, zeros] if h % 2 == 0 else [zeros, q]
        return dot(keys, jnp.concatenate(halves + [pick], axis=0))

    def finish(h, scores):
        top = jnp.max(scores, axis=0, keepdims=True)
        if state_in is not None:
            old = state_in[h, HEAD_DIM + 8 : HEAD_DIM + 9, :]
            top = jnp.maximum(top, old)
        expo = jnp.exp2(scores - top).astype(BF16)
        values = jnp.concatenate([vt[h * HEAD_DIM : (h + 1) * HEAD_DIM, :], ones], axis=0)
        part = dot(values, expo)[: HEAD_DIM + 8]
        if state_in is not None:
            part = part + state_in[h, : HEAD_DIM + 8, :] * jnp.exp2(old - top)
        state_out[h, : HEAD_DIM + 8, :] = part
        state_out[h, HEAD_DIM + 8 :, :] = jnp.broadcast_to(top, (8, tok))

    ahead = score(0)
    for h in range(heads):
        scores = ahead
        if h + 1 < heads:
            ahead = score(h + 1)
        finish(h, scores)


def first_kernel(info, x_ref, wq, wk, wv, qt_ref, state_ref):
    x = x_ref[...]
    scale = math.log2(math.e) / math.sqrt(HEAD_DIM)
    qt_ref[...] = (dot(x, wq[...]) * scale).T.astype(BF16)
    bias = key_bias(info[0] * x.shape[0], info[2], x.shape[0])
    attend_chunk(x, wk[...], wv[...], qt_ref, bias, None, state_ref)


def next_kernel(step, n_seq, info, xr_ref, xl_ref, wk, wv, qt_ref, state_in, state_ref):
    count = xr_ref.shape[0]
    rank = info[0]
    from_left = rank >= step
    from_right = rank + step < n_seq

    def add(x_ref, place, before):
        bias = key_bias(place * count, info[2], count)
        attend_chunk(x_ref[...], wk[...], wv[...], qt_ref, bias, before, state_ref)

    @pl.when(jnp.logical_not(from_left))
    def _():
        state_ref[...] = state_in[...]

    @pl.when(from_left)
    def _():
        add(xr_ref, rank - step, state_in)

    @pl.when(from_right)
    def _():
        add(xl_ref, rank + step, state_ref)


def attend_specs(tok, width):
    cols = HEADS_STEP * HEAD_DIM
    groups = width // cols
    info = pl.BlockSpec(memory_space=pltpu.SMEM)
    full = pl.BlockSpec((tok, width), lambda j: (0, 0))
    weight = [
        pl.BlockSpec((width, cols), functools.partial(lambda s, j: (0, s * groups + j), s))
        for s in range(3)
    ]
    qt = pl.BlockSpec((cols, tok), lambda j: (j, 0))
    state = pl.BlockSpec((HEADS_STEP, ROWS, tok), lambda j: (j, 0, 0))
    return groups, info, full, weight, qt, state


def attend_options(tok, width):
    return dict(
        compiler_params=pltpu.CompilerParams(
            dimension_semantics=("arbitrary",), vmem_limit_bytes=16 * 1024 * 1024
        ),
        cost_estimate=pl.CostEstimate(
            flops=2 * tok * width * width * 3 + 16 * tok * tok * width,
            bytes_accessed=8 * tok * width,
            transcendentals=tok * tok * width // HEAD_DIM,
        ),
    )


def attend_first(x, weight, info):
    tok, width = x.shape
    groups, s_info, s_x, s_w, s_q, s_state = attend_specs(tok, width)
    return pl.pallas_call(
        first_kernel,
        grid=(groups,),
        in_specs=[s_info, s_x] + s_w,
        out_specs=[s_q, s_state],
        out_shape=[
            jax.ShapeDtypeStruct((width, tok), BF16),
            jax.ShapeDtypeStruct((width // HEAD_DIM, ROWS, tok), F32),
        ],
        name="attend_first",
        **attend_options(tok, width),
    )(info, x, weight, weight, weight)


def attend_next(xr, xl, weight, qt, state, info, step, n_seq):
    tok, width = xr.shape
    groups, s_info, s_x, s_w, s_q, s_state = attend_specs(tok, width)
    return pl.pallas_call(
        functools.partial(next_kernel, step, n_seq),
        grid=(groups,),
        in_specs=[s_info, s_x, s_x, s_w[1], s_w[2], s_q, s_state],
        out_specs=s_state,
        out_shape=jax.ShapeDtypeStruct(state.shape, F32),
        **attend_options(tok, width),
    )(info, xr, xl, weight, weight, qt, state)


def layer_norm(values, gain, shift):
    average = jnp.mean(values, axis=-1, keepdims=True)
    centred = values - average
    variance = jnp.mean(centred * centred, axis=-1, keepdims=True)
    return centred * lax.rsqrt(variance + EPS) * gain + shift


def mixed_norm(state_ref, wo, x_ref, gain, shift):
    columns = []
    for h in range(state_ref.shape[0]):
        block = state_ref[h]
        columns.append(block[:HEAD_DIM] / block[HEAD_DIM : HEAD_DIM + 1])
    attended = jnp.concatenate(columns, axis=0).T.astype(BF16)
    mixed = dot(attended, wo[...]) + x_ref[...].astype(F32)
    return layer_norm(mixed, gain[...], shift[...]).astype(BF16)


def feed_kernel(masks, info, state_ref, wo, x_ref, gain1, shift1, gain2, shift2, *refs):
    count = len(masks)
    ups, downs = refs[:count], refs[count : 2 * count]
    out_ref, pooled_ref, inner, normed, parts_in, parts_out = refs[2 * count :]
    tok, _ = normed.shape
    rows, ff = ups[0].shape
    cols = min(512, ff)
    owner = [jnp.bitwise_xor(info[1], m) for m in masks]
    normed[...] = mixed_norm(state_ref, wo, x_ref, gain1, shift1)
    for j in range(count):
        parts_in[j] = normed[:, j * rows : (j + 1) * rows]
    lhs = jnp.concatenate([parts_in[o] for o in owner], axis=1)
    for c in range(0, ff, cols):
        pre = dot(lhs, jnp.concatenate([u[:, c : c + cols] for u in ups], axis=0))
        inner[:, c : c + cols] = (0.5 * pre * (1.0 + lax.erf(pre * math.sqrt(0.5)))).astype(BF16)
    per = max(1, 256 // rows)
    for i in range(0, count, per):
        piece = lax.dot_general(
            inner[...],
            jnp.concatenate([d[...] for d in downs[i : i + per]], axis=0),
            (((1,), (1,)), ((), ())),
            preferred_element_type=F32,
        )
        for n, o in enumerate(owner[i : i + per]):
            parts_out[o] = piece[:, n * rows : (n + 1) * rows]
    outer = jnp.concatenate([parts_out[j] for j in range(count)], axis=1)
    final = layer_norm(outer + normed[...].astype(F32), gain2[...], shift2[...])
    out_ref[...] = final.astype(BF16)
    place = info[0] * tok + lax.broadcasted_iota(jnp.int32, (tok, 1), 0)
    total = jnp.sum(jnp.where(place < info[2], final, 0.0), axis=0, keepdims=True)
    pooled_ref[...] = total / info[2].astype(F32)


def feed(state, wo, x, norms, ups, downs, masks, info):
    tok, width = x.shape
    rows, ff = ups[0].shape
    vmem = pl.BlockSpec(memory_space=pltpu.VMEM)
    return pl.pallas_call(
        functools.partial(feed_kernel, masks),
        in_specs=[pl.BlockSpec(memory_space=pltpu.SMEM)] + [vmem] * (7 + 2 * len(masks)),
        out_specs=[vmem, vmem],
        out_shape=[
            jax.ShapeDtypeStruct((tok, width), BF16),
            jax.ShapeDtypeStruct((1, width), F32),
        ],
        scratch_shapes=[
            pltpu.VMEM((tok, ff), BF16),
            pltpu.VMEM((tok, width), BF16),
            pltpu.VMEM((len(masks), tok, rows), BF16),
            pltpu.VMEM((len(masks), tok, rows), F32),
        ],
        compiler_params=pltpu.CompilerParams(vmem_limit_bytes=16 * 1024 * 1024),
        cost_estimate=pl.CostEstimate(
            flops=2 * tok * width * (width + 2 * ff),
            bytes_accessed=4 * width * ff,
            transcendentals=tok * ff,
        ),
        name="feed",
    )(info, state, wo, x, *norms, *ups, *downs)


def gather_rows(part, axis, size, first):
    bits = [1 << b for b in range(size.bit_length() - 1)]

    def swap(values, mask):
        return lax.ppermute(values, axis, [(i, i ^ mask) for i in range(size)])

    found = {0: part}
    rest = bits
    if len(bits) >= 3:
        links = bits[1:3]
        rest = [b for b in bits if b not in links]
        for bit in links:
            found[bit] = swap(part, bit)
        found[links[0] | links[1]] = swap(found[links[1 - first]], links[first])
    for bit in rest:
        for m in list(found):
            found[m | bit] = swap(found[m], bit)
    masks = sorted(found)
    return tuple(masks), [found[m] for m in masks]


def sum_axis(values, axis, size):
    bit = 1
    while bit < size:
        pairs = [(i, i ^ bit) for i in range(size)]
        values = values + lax.ppermute(values, axis, pairs)
        bit *= 2
    return values


def line_shift(values, axis, size, step):
    pairs = [(i, i + step) for i in range(size) if 0 <= i + step < size]
    return lax.ppermute(values, axis, pairs)


def body(
    n_seq,
    n_grp,
    hidden_in,
    lengths,
    project_weight,
    output_weight,
    first_gain,
    first_shift,
    up_weight,
    down_weight,
    second_gain,
    second_shift,
    queries,
    positive,
):
    tokens = hidden_in[0]
    rank = lax.axis_index("seq")
    shard = lax.axis_index("grp")
    length = lengths[0]

    info = jnp.stack([rank, shard, length]).astype(jnp.int32)
    right = left = tokens
    arrived = []
    for _ in range(1, n_seq):
        right = line_shift(right, "seq", n_seq, 1)
        left = line_shift(left, "seq", n_seq, -1)
        arrived.append((right, left))
    masks, ups = gather_rows(up_weight, "grp", n_grp, 0)
    _, downs = gather_rows(down_weight, "grp", n_grp, 1)

    qt, state = attend_first(tokens, project_weight, info)
    for step, (right, left) in enumerate(arrived, 1):
        state = attend_next(right, left, project_weight, qt, state, info, step, n_seq)
    norms = [v[None] for v in (first_gain, first_shift, second_gain, second_shift)]
    final, part = feed(state, output_weight, tokens, norms, ups, downs, masks, info)
    pooled = sum_axis(part, "seq", n_seq)
    embedding = pooled / jnp.sqrt(jnp.sum(pooled * pooled) + 1e-06)
    short_passages = lax.all_gather(embedding.astype(BF16), "grp", axis=0, tiled=True)
    short_queries = (
        queries / jnp.sqrt(jnp.sum(queries * queries, axis=-1, keepdims=True) + 1e-06)
    ).astype(BF16)
    logits = 20.0 * jnp.dot(short_queries, short_passages.T, preferred_element_type=F32)
    passage_ids = jnp.arange(short_passages.shape[0], dtype=jnp.int32)
    chosen = positive[:, None] == passage_ids[None, :]
    picked = jnp.sum(jnp.where(chosen, logits, 0.0), axis=1)
    query_loss = jnp.log(jnp.sum(jnp.exp(logits), axis=1)) - picked
    return (final[None], embedding, query_loss)


def solution(mesh):
    in_specs = (
        P("grp", "seq", None),
        P("grp"),
        P(),
        P(),
        P(),
        P(),
        P("grp", None),
        P("grp", None),
        P(),
        P(),
        P("grp", None),
        P("grp"),
    )
    out_specs = (P("grp", "seq", None), P("grp", None), P("grp"))

    def run(*args):
        return body(mesh.shape["seq"], mesh.shape["grp"], *args)

    return jax.shard_map(run, mesh=mesh, in_specs=in_specs, out_specs=out_specs, check_vma=False)
```
